32 devices in a mesh: rep: 1, dp: 32 (over x, y, z, core).
Axes of the slice: x: 2, y: 2, z: 4, core: 2. Of those that a mesh axis runs over, the one named last changes fastest.
Arguments:
- g_w_gate: bfloat16 [32, 2, 1024, 3200], P(('rep', 'dp'))
- g_w_up: bfloat16 [32, 2, 1024, 3200], P(('rep', 'dp'))
- g_w_down: bfloat16 [32, 2, 3200, 1024], P(('rep', 'dp'))
- w_gate: bfloat16 [2, 1024, 3200], replicated
- w_up: bfloat16 [2, 1024, 3200], replicated
- w_down: bfloat16 [2, 3200, 1024], replicated
- m_w_gate: float32 [2, 1024, 3200], P(None, 'dp')
- m_w_up: float32 [2, 1024, 3200], P(None, 'dp')
- m_w_down: float32 [2, 3200, 1024], P(None, 'dp')
- v_w_gate: float32 [2, 1024, 3200], P(None, 'dp')
- v_w_up: float32 [2, 1024, 3200], P(None, 'dp')
- v_w_down: float32 [2, 3200, 1024], P(None, 'dp')
Outputs:
- output 1: bfloat16 [2, 1024, 3200], P('rep')
- output 2: bfloat16 [2, 1024, 3200], P('rep')
- output 3: bfloat16 [2, 3200, 1024], P('rep')
- output 4: float32 [2, 1024, 3200], P('rep', 'dp')
- output 5: float32 [2, 1024, 3200], P('rep', 'dp')
- output 6: float32 [2, 3200, 1024], P('rep', 'dp')
- output 7: float32 [2, 1024, 3200], P('rep', 'dp')
- output 8: float32 [2, 1024, 3200], P('rep', 'dp')
- output 9: float32 [2, 3200, 1024], P('rep', 'dp')
All inputs are finite; a program needn't handle non-finite values.
Results may differ from the reference program's by a relative error of at most 0.022.
Values are sent between devices in bfloat16 or wider.
A program may use at most 2 GiB of HBM per device.

```python
import jax
import jax.numpy as jnp
from jax import lax

DEVICES = 32
D = 1024
FF = 3200
LAYERS = 2
NAMES = ("w_gate", "w_up", "w_down")
SHAPES = {"w_gate": (LAYERS, D, FF), "w_up": (LAYERS, D, FF), "w_down": (LAYERS, FF, D)}


def setup_inputs(seed: int = 0, part: int = 0) -> dict:
    kz, *keys = jax.random.split(jax.random.key(seed), 1 + 5 * len(NAMES))
    loud = 2.0 ** jax.random.uniform(kz, (), jnp.float32, -1.0, 1.0)
    drawn = {}
    for name, key, both in zip(NAMES, keys[:3], keys[3:6], strict=True):
        own = jax.random.normal(jax.random.fold_in(key, part), (DEVICES, *SHAPES[name]), jnp.float32)
        shared = jax.random.normal(jax.random.fold_in(both, part), SHAPES[name], jnp.float32)
        drawn["g_" + name] = (loud * (0.7 * shared / DEVICES + 0.7 * own * DEVICES**-0.5)).astype(jnp.bfloat16)
    for name, key in zip(NAMES, keys[6:9], strict=True):
        drawn[name] = (jax.random.normal(key, SHAPES[name], jnp.float32) * SHAPES[name][1] ** -0.5).astype(jnp.bfloat16)
    for name, key in zip(NAMES, keys[9:12], strict=True):
        drawn["m_" + name] = loud * 0.5 * jax.random.normal(key, SHAPES[name], jnp.float32)
    for name, key in zip(NAMES, keys[12:15], strict=True):
        drawn["v_" + name] = loud * loud * jax.random.uniform(key, SHAPES[name], jnp.float32, 0.5, 1.5)
    return drawn


def adamw(w, m, v, g):
    m = 0.9 * m + 0.1 * g
    v = 0.95 * v + 0.05 * g * g
    step = m * lax.rsqrt(v + 1e-8) + 0.1 * w
    return (w - 0.02 * step).astype(jnp.bfloat16), m, v


def clipped(gradients, sum_of_squares, count):
    factor = jnp.minimum(1.0, 0.5 * lax.rsqrt(sum_of_squares / count + 1e-30))
    return [g * factor for g in gradients]


def reference(g_w_gate, g_w_up, g_w_down, w_gate, w_up, w_down, m_w_gate, m_w_up, m_w_down, v_w_gate, v_w_up, v_w_down):
    def total(terms):
        return lax.scan(lambda so_far, term: (so_far + term.astype(jnp.float32), None), jnp.zeros(terms.shape[1:], jnp.float32), terms)[0]

    gradients = [total(terms).astype(jnp.bfloat16).astype(jnp.float32) for terms in (g_w_gate, g_w_up, g_w_down)]
    gradients = clipped(gradients, sum(jnp.sum(g * g) for g in gradients), sum(g.size for g in gradients))
    new = [
        adamw(w.astype(jnp.float32), m, v, g)
        for w, m, v, g in zip((w_gate, w_up, w_down), (m_w_gate, m_w_up, m_w_down), (v_w_gate, v_w_up, v_w_down), gradients, strict=True)
    ]
    return tuple(one[which] for which in range(3) for one in new)
```

```python
import functools
import itertools

import jax
import jax.numpy as jnp
from jax import lax
from jax.experimental import pallas as pl
from jax.experimental.pallas import tpu as pltpu
from jax.sharding import PartitionSpec as P

MESH = pl.DeviceIdType.MESH
F32, BF16 = jnp.float32, jnp.bfloat16

X, Y, Z1, Z0 = range(4)
CHIP_BITS = (16, 8, 4, 2)
ORDERS = ((X, Y, Z0, Z1), (Y, Z0, X, Z1), (Z0, X, Y, Z1))
STEP_OF = {s: 4 - s.bit_length() for s in range(1, 16)}


def adamw(w, m, v, g):
    m = 0.9 * m + 0.1 * g
    v = 0.95 * v + 0.05 * g * g
    step = m * lax.rsqrt(v + 1e-8) + 0.1 * w
    return (w - 0.02 * step).astype(BF16), m, v


class Place:
    def __init__(self):
        me = lax.axis_index("dp")
        self.core = lax.rem(me, 2)
        self.other = 1 - self.core
        self.bits = [lax.rem(lax.div(me, bit), 2) for bit in CHIP_BITS]
        self.partner = [{"dp": me + bit * (1 - 2 * b)} for bit, b in zip(CHIP_BITS, self.bits)]
        self.mate = {"dp": me + 1 - 2 * self.core}

    def block(self, order, slot):
        at = list(self.bits)
        for step, bit in enumerate(order):
            if slot >> (3 - step) & 1:
                at[bit] = 1 - at[bit]
        return tuple(at)

    def greet(self):
        barrier = pltpu.get_barrier_semaphore()
        for device in (*self.partner, self.mate):
            pl.semaphore_signal(barrier, inc=1, device_id=device, device_id_type=MESH)
        pl.semaphore_wait(barrier, 5)


def remote(src, dst, send, recv, device):
    return pltpu.make_async_remote_copy(src_ref=src, dst_ref=dst, send_sem=send, recv_sem=recv, device_id=device, device_id_type=MESH)


def pieces(shape):
    rows, columns = shape
    if rows % 16 == 0:
        return rows // 16, lambda i: (pl.ds(pl.multiple_of(i * 16, 16), 16), slice(None))
    return columns // 128, lambda i: (slice(None), pl.ds(pl.multiple_of(i * 128, 128), 128))


def sum_kernel(*refs):
    n = len(ORDERS)
    refs = iter(refs)
    take = lambda: [next(refs) for _ in range(n)]
    terms, sums, (squares,) = take(), take(), [next(refs)]
    own, mate, got = take(), take(), take()
    partial, own_sem, mate_send, mate_recv, send, recv, out_send, out_recv, sq_send, sq_recv = refs
    here = Place()
    core, other = here.core, here.other
    here.greet()

    def own_copy(w, s):
        at = here.block(ORDERS[w], s)
        return pltpu.make_async_copy(terms[w].at[(core, *at)], own[w].at[s], own_sem.at[w, s])

    def mate_copy(w, s):
        at = here.block(ORDERS[w], s)
        return remote(terms[w].at[(other, *at)], mate[w].at[s], mate_send.at[w, s], mate_recv.at[w, s], here.mate)

    def hop(w, s):
        return remote(own[w].at[s], got[w].at[s], send.at[w, s], recv.at[w, s], here.partner[ORDERS[w][STEP_OF[s]]])

    everything = list(itertools.product(reversed(range(16)), range(n)))
    for s, w in everything:
        mate_copy(w, s).start()
        own_copy(w, s).start()

    squares[...] = jnp.zeros_like(squares)
    for s, w in everything:
        own_copy(w, s).wait()
        mate_copy(w, s).wait_recv()
        arrived = [s + b for b in (8, 4, 2, 1) if s < b]
        for a in arrived:
            hop(w, a).wait_recv()
        count, piece = pieces(own[w].shape[1:])

        def total(i):
            at = (s, *piece(i))
            so_far = own[w][at].astype(F32) + mate[w][at].astype(F32)
            for a in arrived:
                so_far = so_far + got[w][(a, *piece(i))].astype(F32)
            return so_far.astype(BF16)

        if s:

            def body(i, _):
                own[w][(s, *piece(i))] = total(i)
                return _

            lax.fori_loop(0, count, body, 0)
            hop(w, s).start()
        else:

            def body(i, _):
                value = total(i)
                sums[w][(core, *piece(i))] = value
                value = value.astype(F32)
                squares[...] += jnp.sum(value * value)
                return _

            lax.fori_loop(0, count, body, 0)
            remote(sums[w].at[core], sums[w].at[core], out_send.at[w], out_recv.at[w], here.mate).start()

    for i, device in enumerate((here.mate, *here.partner)):
        partial[i] = squares[...]
        copy = remote(partial.at[i], partial.at[5 + i], sq_send.at[i], sq_recv.at[i], device)
        copy.start()
        copy.wait()
        squares[...] += partial[5 + i]

    for w in range(n):
        remote(sums[w].at[other], sums[w].at[other], out_send.at[w], out_recv.at[w], here.mate).wait_recv()
        remote(sums[w].at[core], sums[w].at[core], out_send.at[w], out_recv.at[w], here.mate).wait_send()
    for s, w in everything:
        mate_copy(w, s).wait_send()
        if s:
            hop(w, s).wait_send()


def gather_kernel(*refs):
    n = len(ORDERS)
    refs = iter(refs)
    take = lambda: [next(refs) for _ in range(n)]
    rows, whole, theirs, block = take(), take(), take(), take()
    wide, row_send, row_recv, send, recv, mate_send, mate_recv, own_sem = refs
    here = Place()
    core, other = here.core, here.other
    here.greet()

    def swap(w):
        return remote(rows[w].at[other], theirs[w], row_send.at[w], row_recv.at[w], here.mate)

    def source(w, s):
        return block[w] if s == 0 else whole[w].at[(core, *here.block(ORDERS[w], s))]

    def hop(w, s, step):
        a = s + (8 >> step)
        target = whole[w].at[(core, *here.block(ORDERS[w], s))]
        return remote(source(w, s), target, send.at[w, a], recv.at[w, a], here.partner[ORDERS[w][step]])

    def arrival(w, s):
        target = whole[w].at[(core, *here.block(ORDERS[w], s))]
        return remote(target, target, send.at[w, s], recv.at[w, s], here.partner[ORDERS[w][STEP_OF[s]]])

    def across(w, s):
        target = whole[w].at[(core, *here.block(ORDERS[w], s))]
        return remote(source(w, s), target, mate_send.at[w, s], mate_recv.at[w, s], here.mate)

    def from_across(w, s):
        target = whole[w].at[(other, *here.block(ORDERS[w], s))]
        return remote(target, target, mate_send.at[w, s], mate_recv.at[w, s], here.mate)

    def keep(w):
        return pltpu.make_async_copy(block[w], whole[w].at[(core, *here.bits)], own_sem.at[w])

    for w in range(n):
        swap(w).start()
    for w in range(n):
        swap(w).wait_recv()
        half = rows[w].shape[1]
        mine, his = rows[w][core], theirs[w][...]
        low, high = jnp.where(core == 0, mine, his), jnp.where(core == 0, his, mine)
        if half % 16 == 0:
            block[w][:half] = low
            block[w][half:] = high
        else:
            wide[:half] = low.astype(F32)
            wide[half:] = high.astype(F32)
            block[w][...] = wide[...].astype(BF16)
        for step in reversed(range(4)):
            hop(w, 0, step).start()
        across(w, 0).start()
        keep(w).start()
    for s in range(1, 16):
        for w in range(n):
            arrival(w, s).wait_recv()
            for step in reversed(range(STEP_OF[s])):
                hop(w, s, step).start()
            across(w, s).start()
    for w in range(n):
        swap(w).wait_send()
        keep(w).wait()
        for s in range(16):
            from_across(w, s).wait_recv()
            across(w, s).wait_send()
            for step in range(STEP_OF[s] if s else 4):
                hop(w, s, step).wait_send()


def dma(*shape):
    return pltpu.SemaphoreType.DMA(shape)


def solution(mesh):
    def summed(terms):
        blocks = [t.shape[5:] for t in terms]
        return pl.pallas_call(
            sum_kernel,
            out_shape=[jax.ShapeDtypeStruct((2, *b), BF16) for b in blocks] + [jax.ShapeDtypeStruct((8, 128), F32)],
            in_specs=[pl.BlockSpec(memory_space=pl.ANY)] * 3,
            out_specs=[pl.BlockSpec(memory_space=pltpu.VMEM)] * 4,
            scratch_shapes=[pltpu.VMEM((16, *b), BF16) for b in blocks] * 3
            + [pltpu.VMEM((10, 8, 128), F32)]
            + [dma(3, 16)] * 5
            + [dma(3)] * 2
            + [dma(5)] * 2,
            compiler_params=pltpu.CompilerParams(collective_id=0, has_side_effects=True, vmem_limit_bytes=67_043_328),
            name="sum_terms",
        )(*terms)

    def gathered(rows):
        blocks = [(2 * r.shape[1], r.shape[2]) for r in rows]
        return pl.pallas_call(
            gather_kernel,
            out_shape=[jax.ShapeDtypeStruct((2, 2, 2, 2, 2, *b), BF16) for b in blocks],
            in_specs=[pl.BlockSpec(memory_space=pltpu.VMEM)] * 3,
            out_specs=[pl.BlockSpec(memory_space=pl.ANY)] * 3,
            scratch_shapes=[pltpu.VMEM(r.shape[1:], BF16) for r in rows]
            + [pltpu.VMEM(b, BF16) for b in blocks]
            + [pltpu.VMEM(blocks[2], F32)]
            + [dma(3)] * 2
            + [dma(3, 16)] * 4
            + [dma(3)],
            compiler_params=pltpu.CompilerParams(collective_id=1, has_side_effects=True, vmem_limit_bytes=32 * 2**20),
            name="gather_weights",
        )(*rows)

    def step(*arrays):
        terms, weights, m, v = (arrays[i : i + 3] for i in (0, 3, 6, 9))
        me = lax.axis_index("dp")
        core = lax.rem(me, 2)
        *sums, squares = summed([t[0].reshape(2, 2, 2, 2, 2, -1, t.shape[3]) for t in terms])
        count = sum(w.size for w in weights)
        factor = jnp.minimum(1.0, 0.5 * lax.rsqrt(squares[0, 0] / count + 1e-30))

        def cut(array, index, size):
            return lax.dynamic_slice_in_dim(array, index * size, size, 1).astype(F32)

        new = [adamw(cut(w, me, m.shape[1]), m, v, cut(g, core, m.shape[1]) * factor) for w, m, v, g in zip(weights, m, v, sums, strict=True)]
        whole = [one.reshape(w.shape) for one, w in zip(gathered([one[0] for one in new]), weights, strict=True)]
        return (*whole, *(one[1] for one in new), *(one[2] for one in new))

    all_of, cut_of = P(None, None, None), P(None, "dp", None)
    return jax.shard_map(
        step,
        mesh=mesh,
        in_specs=(P(("rep", "dp"), None, None, None),) * 3 + (all_of,) * 3 + (cut_of,) * 6,
        out_specs=(P("rep", None, None),) * 3 + (P("rep", "dp", None),) * 6,
        check_vma=False,
    )
```

```python
import functools
import itertools

import jax
import jax.numpy as jnp
from jax import lax
from jax.experimental import pallas as pl
from jax.experimental.pallas import tpu as pltpu
from jax.sharding import PartitionSpec as P

MESH = pl.DeviceIdType.MESH
F32, BF16 = jnp.float32, jnp.bfloat16

X, Y, Z1, Z0 = range(4)
CHIP_BITS = (16, 8, 4, 2)
STREAMS = ((0, None, (X, Y, Z0, Z1)), (1, None, (Y, X, Z0, Z1)), (2, 0, (Z0, X, Y, Z1)), (2, 1, (Z0, Y, X, Z1)))
ORDERS = [order for _, _, order in STREAMS]
SLOTS = (15, 13, 11, 9, 7, 5, 14, 3, 12, 1, 10, 8, 6, 4, 2, 0)
STEP_OF = {s: 4 - s.bit_length() for s in range(1, 16)}


def adamw(w, m, v, g):
    m = 0.9 * m + 0.1 * g
    v = 0.95 * v + 0.05 * g * g
    step = m * lax.rsqrt(v + 1e-8) + 0.1 * w
    return (w - 0.02 * step).astype(BF16), m, v


class Place:
    def __init__(self):
        me = lax.axis_index("dp")
        self.core = lax.rem(me, 2)
        self.other = 1 - self.core
        self.bits = [lax.rem(lax.div(me, bit), 2) for bit in CHIP_BITS]
        self.partner = [{"dp": me + bit * (1 - 2 * b)} for bit, b in zip(CHIP_BITS, self.bits)]
        self.mate = {"dp": me + 1 - 2 * self.core}

    def block(self, order, slot):
        at = list(self.bits)
        for step, bit in enumerate(order):
            if slot >> (3 - step) & 1:
                at[bit] = 1 - at[bit]
        return tuple(at)

    def greet(self):
        barrier = pltpu.get_barrier_semaphore()
        for device in (*self.partner, self.mate):
            pl.semaphore_signal(barrier, inc=1, device_id=device, device_id_type=MESH)
        pl.semaphore_wait(barrier, 5)


def columns(part, shape):
    half = shape[1] // 2
    return slice(None) if part is None else pl.ds(part * half, half)


def part_shape(part, shape):
    return shape if part is None else (shape[0], shape[1] // 2)


def remote(src, dst, send, recv, device):
    return pltpu.make_async_remote_copy(src_ref=src, dst_ref=dst, send_sem=send, recv_sem=recv, device_id=device, device_id_type=MESH)


def pieces(shape):
    rows, columns = shape
    if rows % 16 == 0:
        return rows // 16, lambda i: (pl.ds(pl.multiple_of(i * 16, 16), 16), slice(None))
    return columns // 128, lambda i: (slice(None), pl.ds(pl.multiple_of(i * 128, 128), 128))


def sum_kernel(*refs):
    n = len(STREAMS)
    refs = iter(refs)
    take = lambda count: [next(refs) for _ in range(count)]
    terms, sums, (squares,) = take(3), take(3), take(1)
    own, mate, got = take(n), take(n), take(n)
    partial, own_sem, mate_send, mate_recv, send, recv, out_send, out_recv, sq_send, sq_recv = refs
    here = Place()
    core, other = here.core, here.other
    here.greet()

    def term(w, layer, s):
        which, part, order = STREAMS[w]
        ref = terms[which]
        return ref.at[(layer, *here.block(order, s), slice(None), columns(part, ref.shape[5:]))]

    def own_copy(w, s):
        return pltpu.make_async_copy(term(w, core, s), own[w].at[s], own_sem.at[w, s])

    def mate_copy(w, s):
        return remote(term(w, other, s), mate[w].at[s], mate_send.at[w, s], mate_recv.at[w, s], here.mate)

    def result(w, layer):
        which, part, _ = STREAMS[w]
        ref = sums[which].at[layer, :, columns(part, sums[which].shape[1:])]
        return ref

    def swap(w, layer):
        return remote(result(w, layer), result(w, layer), out_send.at[w], out_recv.at[w], here.mate)

    def hop(w, s):
        return remote(own[w].at[s], got[w].at[s], send.at[w, s], recv.at[w, s], here.partner[ORDERS[w][STEP_OF[s]]])

    everything = list(itertools.product(SLOTS, range(n)))
    for s, w in everything:
        mate_copy(w, s).start()
        own_copy(w, s).start()

    squares[...] = jnp.zeros_like(squares)
    for s, w in everything:
        own_copy(w, s).wait()
        mate_copy(w, s).wait_recv()
        arrived = [s + b for b in (8, 4, 2, 1) if s < b]
        for a in arrived:
            hop(w, a).wait_recv()
        count, piece = pieces(own[w].shape[1:])

        def total(i):
            at = (s, *piece(i))
            so_far = own[w][at].astype(F32) + mate[w][at].astype(F32)
            for a in arrived:
                so_far = so_far + got[w][(a, *piece(i))].astype(F32)
            return so_far.astype(BF16)

        if s:

            def body(i, _):
                own[w][(s, *piece(i))] = total(i)
                return _

            lax.fori_loop(0, count, body, 0)
            hop(w, s).start()
        else:

            def body(i, _):
                value = total(i)
                target = result(w, core)
                target[piece(i)] = value
                value = value.astype(F32)
                squares[...] += jnp.sum(value * value)
                return _

            lax.fori_loop(0, count, body, 0)
            swap(w, core).start()

    for i, device in enumerate((here.mate, *here.partner)):
        partial[i] = squares[...]
        copy = remote(partial.at[i], partial.at[5 + i], sq_send.at[i], sq_recv.at[i], device)
        copy.start()
        copy.wait()
        squares[...] += partial[5 + i]

    for w in range(n):
        swap(w, other).wait_recv()
        swap(w, core).wait_send()
    for s, w in everything:
        mate_copy(w, s).wait_send()
        if s:
            hop(w, s).wait_send()


def gather_kernel(*refs):
    n = len(STREAMS)
    refs = iter(refs)
    take = lambda: [next(refs) for _ in range(3)]
    rows, whole, theirs, block = take(), take(), take(), take()
    wide, row_send, row_recv, send, recv, mate_send, mate_recv, own_sem = refs
    here = Place()
    core, other = here.core, here.other
    here.greet()

    def swap(w):
        return remote(rows[w].at[other], theirs[w], row_send.at[w], row_recv.at[w], here.mate)

    def place(w, s, layer):
        which, part, order = STREAMS[w]
        ref = whole[which]
        return ref.at[(layer, *here.block(order, s), slice(None), columns(part, ref.shape[5:]))]

    def source(w, s):
        which, part, _ = STREAMS[w]
        return place(w, s, core) if s else block[which].at[:, columns(part, block[which].shape)]

    def hop(w, s, step):
        a = s + (8 >> step)
        return remote(source(w, s), place(w, s, core), send.at[w, a], recv.at[w, a], here.partner[ORDERS[w][step]])

    def arrival(w, s):
        target = place(w, s, core)
        return remote(target, target, send.at[w, s], recv.at[w, s], here.partner[ORDERS[w][STEP_OF[s]]])

    def across(w, s):
        return remote(source(w, s), place(w, s, core), mate_send.at[w, s], mate_recv.at[w, s], here.mate)

    def from_across(w, s):
        target = place(w, s, other)
        return remote(target, target, mate_send.at[w, s], mate_recv.at[w, s], here.mate)

    def keep(w):
        return pltpu.make_async_copy(block[w], whole[w].at[(core, *here.bits)], own_sem.at[w])

    for w in range(3):
        swap(w).start()
    for w in range(3):
        swap(w).wait_recv()
        half = rows[w].shape[1]
        mine, his = rows[w][core], theirs[w][...]
        low, high = jnp.where(core == 0, mine, his), jnp.where(core == 0, his, mine)
        if half % 16 == 0:
            block[w][:half] = low
            block[w][half:] = high
        else:
            wide[:half] = low.astype(F32)
            wide[half:] = high.astype(F32)
            block[w][...] = wide[...].astype(BF16)
        for stream in range(n):
            if STREAMS[stream][0] == w:
                for step in (2, 1, 0):
                    hop(stream, 0, step).start()
    for stream in range(n):
        hop(stream, 0, 3).start()
    for stream in range(n):
        across(stream, 0).start()
    for w in range(3):
        keep(w).start()
    for s in reversed(SLOTS[:-1]):
        for w in range(n):
            arrival(w, s).wait_recv()
            for step in reversed(range(STEP_OF[s])):
                hop(w, s, step).start()
            across(w, s).start()
    for w in range(3):
        swap(w).wait_send()
        keep(w).wait()
    for w in range(n):
        for s in range(16):
            from_across(w, s).wait_recv()
            across(w, s).wait_send()
            for step in range(STEP_OF[s] if s else 4):
                hop(w, s, step).wait_send()


def dma(*shape):
    return pltpu.SemaphoreType.DMA(shape)


def solution(mesh):
    def summed(terms):
        blocks = [t.shape[5:] for t in terms]
        return pl.pallas_call(
            sum_kernel,
            out_shape=[jax.ShapeDtypeStruct((2, *b), BF16) for b in blocks] + [jax.ShapeDtypeStruct((8, 128), F32)],
            in_specs=[pl.BlockSpec(memory_space=pl.ANY)] * 3,
            out_specs=[pl.BlockSpec(memory_space=pltpu.VMEM)] * 4,
            scratch_shapes=[pltpu.VMEM((16, *part_shape(part, blocks[which])), BF16) for which, part, _ in STREAMS] * 3
            + [pltpu.VMEM((10, 8, 128), F32)]
            + [dma(len(STREAMS), 16)] * 5
            + [dma(len(STREAMS))] * 2
            + [dma(5)] * 2,
            compiler_params=pltpu.CompilerParams(collective_id=0, has_side_effects=True, vmem_limit_bytes=67_043_328),
            name="sum_terms",
        )(*terms)

    def gathered(rows):
        blocks = [(2 * r.shape[1], r.shape[2]) for r in rows]
        return pl.pallas_call(
            gather_kernel,
            out_shape=[jax.ShapeDtypeStruct((2, 2, 2, 2, 2, *b), BF16) for b in blocks],
            in_specs=[pl.BlockSpec(memory_space=pltpu.VMEM)] * 3,
            out_specs=[pl.BlockSpec(memory_space=pl.ANY)] * 3,
            scratch_shapes=[pltpu.VMEM(r.shape[1:], BF16) for r in rows]
            + [pltpu.VMEM(b, BF16) for b in blocks]
            + [pltpu.VMEM(blocks[2], F32)]
            + [dma(3)] * 2
            + [dma(len(STREAMS), 16)] * 4
            + [dma(3)],
            compiler_params=pltpu.CompilerParams(collective_id=1, has_side_effects=True, vmem_limit_bytes=32 * 2**20),
            name="gather_weights",
        )(*rows)

    def step(*arrays):
        terms, weights, m, v = (arrays[i : i + 3] for i in (0, 3, 6, 9))
        me = lax.axis_index("dp")
        core = lax.rem(me, 2)
        *sums, squares = summed([t[0].reshape(2, 2, 2, 2, 2, -1, t.shape[3]) for t in terms])
        count = sum(w.size for w in weights)
        factor = jnp.minimum(1.0, 0.5 * lax.rsqrt(squares[0, 0] / count + 1e-30))

        def cut(array, index, size):
            return lax.dynamic_slice_in_dim(array, index * size, size, 1).astype(F32)

        new = [adamw(cut(w, me, m.shape[1]), m, v, cut(g, core, m.shape[1]) * factor) for w, m, v, g in zip(weights, m, v, sums, strict=True)]
        whole = [one.reshape(w.shape) for one, w in zip(gathered([one[0] for one in new]), weights, strict=True)]
        return (*whole, *(one[1] for one in new), *(one[2] for one in new))

    all_of, cut_of = P(None, None, None), P(None, "dp", None)
    return jax.shard_map(
        step,
        mesh=mesh,
        in_specs=(P(("rep", "dp"), None, None, None),) * 3 + (all_of,) * 3 + (cut_of,) * 6,
        out_specs=(P("rep", None, None),) * 3 + (P("rep", "dp", None),) * 6,
        check_vma=False,
    )
```

```python
import functools

import jax
import jax.numpy as jnp
from jax import lax
from jax.experimental import pallas as pl
from jax.experimental.pallas import tpu as pltpu
from jax.sharding import PartitionSpec as P

MESH = pl.DeviceIdType.MESH
F32, BF16 = jnp.float32, jnp.bfloat16

X, Y, Z1, Z0 = range(4)
DEVICES = 32
CHIP_BITS = (16, 8, 4, 2)
STREAMS = ((0, None, (X, Y, Z0, Z1)), (1, None, (Y, X, Z0, Z1)), (2, 0, (Z0, X, Y, Z1)), (2, 1, (Z0, Y, X, Z1)))
ORDERS = [order for _, _, order in STREAMS]
SUM = (
    (3, 15), (1, 15), (0, 15), (2, 10), (2, 9), (1, 14), (0, 11), (3, 10), (3, 13), (0, 7), (2, 15), (3, 11), (2, 12), (2, 14),
    (0, 13), (0, 14), (3, 7), (0, 3), (1, 11), (0, 5), (1, 7), (0, 9), (2, 13), (1, 9), (2, 7), (1, 13), (3, 5), (1, 6), (3, 3),
    (2, 11), (0, 10), (3, 8), (3, 9), (0, 6), (2, 8), (2, 6), (1, 3), (3, 14), (0, 1), (3, 1), (1, 5), (3, 12), (1, 10), (0, 12),
    (2, 4), (2, 3), (1, 12), (0, 2), (1, 2), (2, 5), (1, 1), (3, 6), (1, 8), (2, 2), (0, 4), (0, 8), (1, 4), (2, 1), (3, 2), (3, 4),
    (0, 0), (1, 0), (2, 0), (3, 0),
)
GATHER = (
    (3, None, 1), (0, None, 0), (0, None, 2), (1, None, 0), (3, None, 2), (1, None, 2), (0, None, 1), (3, None, 3), (2, None, 3),
    (2, None, 1), (1, None, 1), (2, None, 2), (3, 1), (0, 2), (2, None, 0), (0, 4), (2, 1), (1, 2), (2, 2), (3, 4), (1, 4),
    (1, None, 3), (3, 2), (1, 1), (3, 3), (2, 3), (0, 12), (0, None, 3), (1, 6), (1, 10), (0, 6), (2, 10), (3, 5), (1, 3), (0, 1),
    (2, 7), (0, 10), (3, None, 0), (3, 7), (0, 3), (2, 6), (0, 5), (0, 8), (1, 9), (1, 5), (0, 7), (1, 12), (1, 14), (2, 5), (2, 14),
    (2, 8), (0, 14), (1, 11), (0, 9), (2, 15), (3, 6), (0, 11), (1, 7), (2, 4), (2, 11), (3, 12), (3, 15), (1, 8), (2, 13), (0, 13),
    (1, 13), (0, 15), (2, 12), (3, 8), (3, 13), (3, 10), (3, 11), (3, 14), (3, 9), (2, 9), (1, 15),
)
STEP_OF = {s: 4 - s.bit_length() for s in range(1, 16)}


def adamw(w, m, v, g):
    m = 0.9 * m + 0.1 * g
    v = 0.95 * v + 0.05 * g * g
    step = m * lax.rsqrt(v + 1e-8) + 0.1 * w
    return (w - 0.02 * step).astype(BF16), m, v


class Place:
    def __init__(self):
        me = self.me = lax.axis_index("dp")
        self.core = lax.rem(me, 2)
        self.other = 1 - self.core
        self.bits = [lax.rem(lax.div(me, bit), 2) for bit in CHIP_BITS]
        self.partner = [{"dp": me + bit * (1 - 2 * b)} for bit, b in zip(CHIP_BITS, self.bits)]
        self.mate = {"dp": me + 1 - 2 * self.core}

    def block(self, order, slot):
        at = list(self.bits)
        for step, bit in enumerate(order):
            if slot >> (3 - step) & 1:
                at[bit] = 1 - at[bit]
        return tuple(at)

    def nth(self, k):
        return {"dp": lax.rem(self.me + k, DEVICES)}

    def greet(self, everyone=False):
        barrier = pltpu.get_barrier_semaphore()
        if everyone:

            def signal(k, _):
                pl.semaphore_signal(barrier, inc=1, device_id=self.nth(k), device_id_type=MESH)
                return _

            lax.fori_loop(1, DEVICES, signal, 0)
            pl.semaphore_wait(barrier, DEVICES - 1)
        else:
            for device in (*self.partner, self.mate):
                pl.semaphore_signal(barrier, inc=1, device_id=device, device_id_type=MESH)
            pl.semaphore_wait(barrier, 5)


def columns(part, shape):
    half = shape[1] // 2
    return slice(None) if part is None else pl.ds(part * half, half)


def part_shape(part, shape):
    return shape if part is None else (shape[0], shape[1] // 2)


def remote(src, dst, send, recv, device):
    return pltpu.make_async_remote_copy(src_ref=src, dst_ref=dst, send_sem=send, recv_sem=recv, device_id=device, device_id_type=MESH)


def pieces(shape):
    rows, columns = shape
    if rows % 16 == 0:
        return rows // 16, lambda i: (pl.ds(pl.multiple_of(i * 16, 16), 16), slice(None))
    return columns // 128, lambda i: (slice(None), pl.ds(pl.multiple_of(i * 128, 128), 128))


def sum_kernel(*refs):
    n = len(STREAMS)
    refs = iter(refs)
    take = lambda count: [next(refs) for _ in range(count)]
    terms, sums, (squares,) = take(3), take(3), take(1)
    own, mate, got = take(n), take(n), take(n)
    parts, own_sem, mate_send, mate_recv, send, recv, out_send, out_recv, sq_send, sq_recv = refs
    here = Place()
    core, other = here.core, here.other
    here.greet(everyone=True)

    def term(w, layer, s):
        which, part, order = STREAMS[w]
        ref = terms[which]
        return ref.at[(layer, *here.block(order, s), slice(None), columns(part, ref.shape[5:]))]

    def own_copy(w, s):
        return pltpu.make_async_copy(term(w, core, s), own[w].at[s], own_sem.at[w, s])

    def mate_copy(w, s):
        return remote(term(w, other, s), mate[w].at[s], mate_send.at[w, s], mate_recv.at[w, s], here.mate)

    def result(w, layer):
        which, part, _ = STREAMS[w]
        ref = sums[which].at[layer, :, columns(part, sums[which].shape[1:])]
        return ref

    def swap(w, layer):
        return remote(result(w, layer), result(w, layer), out_send.at[w], out_recv.at[w], here.mate)

    def hop(w, s):
        return remote(own[w].at[s], got[w].at[s], send.at[w, s], recv.at[w, s], here.partner[ORDERS[w][STEP_OF[s]]])

    for w, s in SUM:
        mate_copy(w, s).start()
        own_copy(w, s).start()

    squares[...] = jnp.zeros_like(squares)
    for w, s in SUM:
        own_copy(w, s).wait()
        mate_copy(w, s).wait_recv()
        arrived = [s + b for b in (8, 4, 2, 1) if s < b]
        for a in arrived:
            hop(w, a).wait_recv()
        count, piece = pieces(own[w].shape[1:])

        def total(i):
            at = (s, *piece(i))
            so_far = own[w][at].astype(F32) + mate[w][at].astype(F32)
            for a in arrived:
                so_far = so_far + got[w][(a, *piece(i))].astype(F32)
            return so_far.astype(BF16)

        if s:

            def body(i, _):
                own[w][(s, *piece(i))] = total(i)
                return _

            lax.fori_loop(0, count, body, 0)
            hop(w, s).start()
        else:

            def body(i, _):
                value = total(i)
                target = result(w, core)
                target[piece(i)] = value
                value = value.astype(F32)
                value = (value * value).reshape(-1, 8, value.shape[1]).sum(0)
                squares[...] += sum(value[:, j : j + 128] for j in range(0, value.shape[1], 128))
                return _

            lax.fori_loop(0, count, body, 0)
            swap(w, core).start()

    me = here.me
    parts[me] = squares[...]

    def part_to(k):
        return remote(parts.at[me], parts.at[me], sq_send.at[k], sq_recv.at[me], here.nth(k))

    def part_from(k):
        peer = lax.rem(me + k, DEVICES)
        return remote(parts.at[peer], parts.at[peer], sq_send.at[k], sq_recv.at[peer], here.nth(k))

    def start(k, _):
        part_to(k).start()
        return _

    def take_in(k, _):
        part_from(k).wait_recv()
        return _

    def drain(k, _):
        part_to(k).wait_send()
        return _

    lax.fori_loop(1, DEVICES, start, 0)
    lax.fori_loop(1, DEVICES, take_in, 0)
    squares[...] = jnp.full_like(squares, jnp.sum(parts[...]))
    lax.fori_loop(1, DEVICES, drain, 0)
    for w in range(n):
        swap(w, other).wait_recv()
        swap(w, core).wait_send()
    for w, s in SUM:
        mate_copy(w, s).wait_send()
        if s:
            hop(w, s).wait_send()


def gather_kernel(*refs):
    n = len(STREAMS)
    refs = iter(refs)
    take = lambda: [next(refs) for _ in range(3)]
    rows, whole, theirs, block = take(), take(), take(), take()
    wide, row_send, row_recv, send, recv, mate_send, mate_recv, own_sem = refs
    here = Place()
    core, other = here.core, here.other
    here.greet()

    def swap(w):
        return remote(rows[w].at[other], theirs[w], row_send.at[w], row_recv.at[w], here.mate)

    def place(w, s, layer):
        which, part, order = STREAMS[w]
        ref = whole[which]
        return ref.at[(layer, *here.block(order, s), slice(None), columns(part, ref.shape[5:]))]

    def source(w, s):
        which, part, _ = STREAMS[w]
        return place(w, s, core) if s else block[which].at[:, columns(part, block[which].shape)]

    def hop(w, s, step):
        a = s + (8 >> step)
        return remote(source(w, s), place(w, s, core), send.at[w, a], recv.at[w, a], here.partner[ORDERS[w][step]])

    def arrival(w, s):
        target = place(w, s, core)
        return remote(target, target, send.at[w, s], recv.at[w, s], here.partner[ORDERS[w][STEP_OF[s]]])

    def across(w, s):
        return remote(source(w, s), place(w, s, core), mate_send.at[w, s], mate_recv.at[w, s], here.mate)

    def from_across(w, s):
        target = place(w, s, other)
        return remote(target, target, mate_send.at[w, s], mate_recv.at[w, s], here.mate)

    def keep(w):
        return pltpu.make_async_copy(block[w], whole[w].at[(core, *here.bits)], own_sem.at[w])

    for w in range(3):
        swap(w).start()
    for w in range(3):
        swap(w).wait_recv()
        half = rows[w].shape[1]
        mine, his = rows[w][core], theirs[w][...]
        low, high = jnp.where(core == 0, mine, his), jnp.where(core == 0, his, mine)
        if half % 16 == 0:
            block[w][:half] = low
            block[w][half:] = high
        else:
            wide[:half] = low.astype(F32)
            wide[half:] = high.astype(F32)
            block[w][...] = wide[...].astype(BF16)
    first = True
    for w, s, *step in GATHER:
        if step:
            hop(w, 0, *step).start()
            continue
        if first:
            for stream in range(n):
                across(stream, 0).start()
            for weight in range(3):
                keep(weight).start()
            first = False
        arrival(w, s).wait_recv()
        for step in reversed(range(STEP_OF[s])):
            hop(w, s, step).start()
        across(w, s).start()
    for w in range(3):
        swap(w).wait_send()
        keep(w).wait()
    for w in range(n):
        for s in range(16):
            from_across(w, s).wait_recv()
            across(w, s).wait_send()
            for step in range(STEP_OF[s] if s else 4):
                hop(w, s, step).wait_send()


def dma(*shape):
    return pltpu.SemaphoreType.DMA(shape)


def solution(mesh):
    def summed(terms):
        blocks = [t.shape[5:] for t in terms]
        return pl.pallas_call(
            sum_kernel,
            out_shape=[jax.ShapeDtypeStruct((2, *b), BF16) for b in blocks] + [jax.ShapeDtypeStruct((8, 128), F32)],
            in_specs=[pl.BlockSpec(memory_space=pl.ANY)] * 3,
            out_specs=[pl.BlockSpec(memory_space=pltpu.VMEM)] * 4,
            scratch_shapes=[pltpu.VMEM((16, *part_shape(part, blocks[which])), BF16) for which, part, _ in STREAMS] * 3
            + [pltpu.VMEM((DEVICES, 8, 128), F32)]
            + [dma(len(STREAMS), 16)] * 5
            + [dma(len(STREAMS))] * 2
            + [dma(DEVICES)] * 2,
            compiler_params=pltpu.CompilerParams(collective_id=0, has_side_effects=True, vmem_limit_bytes=67_043_328),
            name="sum_terms",
        )(*terms)

    def gathered(rows):
        blocks = [(2 * r.shape[1], r.shape[2]) for r in rows]
        return pl.pallas_call(
            gather_kernel,
            out_shape=[jax.ShapeDtypeStruct((2, 2, 2, 2, 2, *b), BF16) for b in blocks],
            in_specs=[pl.BlockSpec(memory_space=pltpu.VMEM)] * 3,
            out_specs=[pl.BlockSpec(memory_space=pl.ANY)] * 3,
            scratch_shapes=[pltpu.VMEM(r.shape[1:], BF16) for r in rows]
            + [pltpu.VMEM(b, BF16) for b in blocks]
            + [pltpu.VMEM(blocks[2], F32)]
            + [dma(3)] * 2
            + [dma(len(STREAMS), 16)] * 4
            + [dma(3)],
            compiler_params=pltpu.CompilerParams(collective_id=1, has_side_effects=True, vmem_limit_bytes=10 * 2**20),
            name="gather_weights",
        )(*rows)

    def step(*arrays):
        terms, weights, m, v = (arrays[i : i + 3] for i in (0, 3, 6, 9))
        me = lax.axis_index("dp")
        core = lax.rem(me, 2)
        *sums, squares = summed([t[0].reshape(2, 2, 2, 2, 2, -1, t.shape[3]) for t in terms])
        count = sum(w.size for w in weights)
        factor = jnp.minimum(1.0, 0.5 * lax.rsqrt(squares[0, 0] / count + 1e-30))

        def cut(array, index, size):
            return lax.dynamic_slice_in_dim(array, index * size, size, 1).astype(F32)

        new = [adamw(cut(w, me, m.shape[1]), m, v, cut(g, core, m.shape[1]) * factor) for w, m, v, g in zip(weights, m, v, sums, strict=True)]
        whole = [one.reshape(w.shape) for one, w in zip(gathered([one[0] for one in new]), weights, strict=True)]
        return (*whole, *(one[1] for one in new), *(one[2] for one in new))

    all_of, cut_of = P(None, None, None), P(None, "dp", None)
    return jax.shard_map(
        step,
        mesh=mesh,
        in_specs=(P(("rep", "dp"), None, None, None),) * 3 + (all_of,) * 3 + (cut_of,) * 6,
        out_specs=(P("rep", None, None),) * 3 + (P("rep", "dp", None),) * 6,
        check_vma=False,
    )
```

```python
import functools

import jax
import jax.numpy as jnp
from jax import lax
from jax.experimental import pallas as pl
from jax.experimental.pallas import tpu as pltpu
from jax.sharding import PartitionSpec as P

MESH = pl.DeviceIdType.MESH
F32, BF16 = jnp.float32, jnp.bfloat16

X, Y, Z1, Z0 = range(4)
DEVICES = 32
CHIP_BITS = (16, 8, 4, 2)
STREAMS = ((0, None, (X, Y, Z0, Z1)), (1, None, (Y, X, Z0, Z1)), (2, 0, (Z0, X, Y, Z1)), (2, 1, (Z0, Y, X, Z1)))
ORDERS = [order for _, _, order in STREAMS]
SUM = (
    61, 29, 15, 9, 63, 43, 31, 55, 59, 11, 46, 57, 13, 62, 40, 26, 7, 53, 47, 51, 23, 45, 30, 5, 39, 3, 14, 60, 49, 42, 21, 27, 38, 58,
    56, 41, 44, 54, 52, 22, 37, 1, 10, 35, 50, 25, 8, 6, 19, 33, 28, 12, 2, 36, 18, 34, 24, 17, 20, 4, 48, 32, 0, 16,
)
GATHER = (
    77, 64, 66, 68, 78, 70, 65, 79, 75, 73, 69, 74, 49, 2, 72, 4, 33, 18, 34, 52, 20, 71, 50, 17, 51, 35, 12, 67, 22, 26, 6, 42, 53,
    19, 1, 39, 10, 76, 55, 3, 38, 5, 8, 25, 21, 7, 28, 30, 37, 46, 40, 14, 27, 9, 47, 54, 11, 23, 36, 43, 60, 63, 24, 45, 13, 29, 15,
    44, 56, 61, 58, 59, 62, 57, 41, 31,
)
SUM = tuple(divmod(entry, 16) for entry in SUM)
GATHER = tuple(divmod(entry, 16) if entry < 64 else (entry // 4 - 16, None, entry % 4) for entry in GATHER)
STEP_OF = {s: 4 - s.bit_length() for s in range(1, 16)}


def adamw(w, m, v, g):
    m = 0.9 * m + 0.1 * g
    v = 0.95 * v + 0.05 * g * g
    step = m * lax.rsqrt(v + 1e-8) + 0.1 * w
    return (w - 0.02 * step).astype(BF16), m, v


class Place:
    def __init__(self):
        me = self.me = lax.axis_index("dp")
        self.core = lax.rem(me, 2)
        self.other = 1 - self.core
        self.bits = [lax.rem(lax.div(me, bit), 2) for bit in CHIP_BITS]
        self.partner = [{"dp": me + bit * (1 - 2 * b)} for bit, b in zip(CHIP_BITS, self.bits)]
        self.mate = {"dp": me + 1 - 2 * self.core}

    def block(self, order, slot):
        at = list(self.bits)
        for step, bit in enumerate(order):
            if slot >> (3 - step) & 1:
                at[bit] = 1 - at[bit]
        return tuple(at)

    def nth(self, k):
        return {"dp": lax.rem(self.me + k, DEVICES)}

    def greet(self):
        barrier = pltpu.get_barrier_semaphore()
        for device in (*self.partner, self.mate):
            pl.semaphore_signal(barrier, inc=1, device_id=device, device_id_type=MESH)
        pl.semaphore_wait(barrier, 5)


def columns(part, shape):
    half = shape[1] // 2
    return slice(None) if part is None else pl.ds(part * half, half)


def part_shape(part, shape):
    return shape if part is None else (shape[0], shape[1] // 2)


def remote(src, dst, send, recv, device):
    return pltpu.make_async_remote_copy(src_ref=src, dst_ref=dst, send_sem=send, recv_sem=recv, device_id=device, device_id_type=MESH)


def pieces(shape):
    rows, columns = shape
    if rows % 16 == 0:
        return rows // 16, lambda i: (pl.ds(pl.multiple_of(i * 16, 16), 16), slice(None))
    return columns // 128, lambda i: (slice(None), pl.ds(pl.multiple_of(i * 128, 128), 128))


def sum_kernel(*refs):
    n = len(STREAMS)
    refs = iter(refs)
    take = lambda count: [next(refs) for _ in range(count)]
    terms, sums, (squares,) = take(3), take(3), take(1)
    own, mate, got, final = take(n), take(n), take(n), take(3)
    parts, own_sem, mate_send, mate_recv, send, recv, out_sem, out_send, out_recv, sq_send, sq_recv = refs
    here = Place()
    core, other = here.core, here.other
    here.greet()

    def term(w, layer, s):
        which, part, order = STREAMS[w]
        ref = terms[which]
        return ref.at[(layer, *here.block(order, s), slice(None), columns(part, ref.shape[5:]))]

    def own_copy(w, s):
        return pltpu.make_async_copy(term(w, core, s), own[w].at[s], own_sem.at[w, s])

    def mate_copy(w, s):
        return remote(term(w, other, s), mate[w].at[s], mate_send.at[w], mate_recv.at[w, s], here.mate)

    def result(w):
        which, part, _ = STREAMS[w]
        return final[which].at[:, columns(part, final[which].shape)]

    def home(w, layer):
        which, part, _ = STREAMS[w]
        return sums[which].at[layer, :, columns(part, final[which].shape)]

    def keep(w):
        return pltpu.make_async_copy(result(w), home(w, core), out_sem.at[w])

    def swap(w):
        return remote(result(w), home(w, core), out_send.at[w], out_recv.at[w], here.mate)

    def from_swap(w):
        return remote(home(w, other), home(w, other), out_send.at[w], out_recv.at[w], here.mate)

    def hop(w, s):
        return remote(own[w].at[s], got[w].at[s], send.at[w], recv.at[w, s], here.partner[ORDERS[w][STEP_OF[s]]])

    for w, s in SUM:
        mate_copy(w, s).start()
        own_copy(w, s).start()

    squares[...] = jnp.zeros_like(squares)
    last = min(SUM.index((w, 0)) for w in range(n))
    for turn, (w, s) in enumerate(SUM):
        if turn == last:
            for stream in range(n):
                remote(mate[stream], mate[stream], mate_send.at[stream], mate_recv.at[stream, 0], here.mate).wait_send()
        own_copy(w, s).wait()
        mate_copy(w, s).wait_recv()
        arrived = [s + b for b in (8, 4, 2, 1) if s < b]
        for a in arrived:
            hop(w, a).wait_recv()
        count, piece = pieces(own[w].shape[1:])

        def total(i):
            at = (s, *piece(i))
            so_far = own[w][at].astype(F32) + mate[w][at].astype(F32)
            for a in arrived:
                so_far = so_far + got[w][(a, *piece(i))].astype(F32)
            return so_far.astype(BF16)

        if s:

            def body(i, _):
                own[w][(s, *piece(i))] = total(i)
                return _

            lax.fori_loop(0, count, body, 0)
            hop(w, s).start()
        else:

            def body(i, _):
                value = total(i)
                target = result(w)
                target[piece(i)] = value
                value = value.astype(F32)
                value = (value * value).reshape(-1, 8, value.shape[1]).sum(0)
                squares[...] += sum(value[:, j : j + 128] for j in range(0, value.shape[1], 128))
                return _

            lax.fori_loop(0, count, body, 0)
            keep(w).start()
            swap(w).start()

    me = here.me
    parts[me] = squares[...]

    def part_to(k):
        return remote(parts.at[me], parts.at[me], sq_send, sq_recv, here.nth(k))

    def start(k, _):
        part_to(k).start()
        return _

    lax.fori_loop(1, DEVICES, start, 0)
    for w in range(n):
        from_swap(w).wait_recv()
        keep(w).wait()
        swap(w).wait_send()
        sent = own[w].at[pl.ds(1, 15)]
        remote(sent, sent, send.at[w], recv.at[w, 0], here.mate).wait_send()
    others = parts.at[pl.ds(0, DEVICES - 1)]
    remote(others, others, sq_send, sq_recv, here.mate).wait()
    squares[...] = jnp.full_like(squares, jnp.sum(parts[...]))


def gather_kernel(*refs):
    n = len(STREAMS)
    refs = iter(refs)
    take = lambda: [next(refs) for _ in range(3)]
    rows, whole, theirs, block = take(), take(), take(), take()
    wide, row_send, row_recv, send, recv, mate_send, mate_recv, own_sem = refs
    here = Place()
    core, other = here.core, here.other
    here.greet()

    def swap(w):
        return remote(rows[w].at[other], theirs[w], row_send.at[w], row_recv.at[w], here.mate)

    def place(w, s, layer):
        which, part, order = STREAMS[w]
        ref = whole[which]
        return ref.at[(layer, *here.block(order, s), slice(None), columns(part, ref.shape[5:]))]

    def source(w, s):
        which, part, _ = STREAMS[w]
        return place(w, s, core) if s else block[which].at[:, columns(part, block[which].shape)]

    def hop(w, s, step):
        a = s + (8 >> step)
        return remote(source(w, s), place(w, s, core), send.at[w, step], recv.at[w, a], here.partner[ORDERS[w][step]])

    def arrival(w, s):
        target = place(w, s, core)
        return remote(target, target, send.at[w, 0], recv.at[w, s], here.partner[ORDERS[w][STEP_OF[s]]])

    def across(w, s):
        return remote(source(w, s), place(w, s, core), mate_send.at[w], mate_recv.at[w], here.mate)

    def blocks_of(w, layer, *cut):
        which, part, _ = STREAMS[w]
        free = (slice(None),) * (5 - len(cut))
        ref = whole[which].at[(layer, *cut, *free, columns(part, whole[which].shape[5:]))]
        return remote(ref, ref, mate_send.at[w], mate_recv.at[w], here.mate), ref

    def keep(w):
        return pltpu.make_async_copy(block[w], whole[w].at[(core, *here.bits)], own_sem.at[w])

    for w in range(3):
        swap(w).start()
    for w in range(3):
        swap(w).wait_recv()
        half = rows[w].shape[1]
        mine, his = rows[w][core], theirs[w][...]
        low, high = jnp.where(core == 0, mine, his), jnp.where(core == 0, his, mine)
        if half % 16 == 0:
            block[w][:half] = low
            block[w][half:] = high
        else:
            wide[:half] = low.astype(F32)
            wide[half:] = high.astype(F32)
            block[w][...] = wide[...].astype(BF16)
    first = True
    for w, s, *step in GATHER:
        if step:
            hop(w, 0, *step).start()
            continue
        if first:
            for stream in range(n):
                across(stream, 0).start()
            for weight in range(3):
                keep(weight).start()
            first = False
        arrival(w, s).wait_recv()
        for step in reversed(range(STEP_OF[s])):
            hop(w, s, step).start()
        across(w, s).start()
    for w in range(3):
        swap(w).wait_send()
        keep(w).wait()
    for w in range(n):
        for step in range(4):
            _, ref = blocks_of(w, core, *[0] * (step + 1))
            remote(ref, ref, send.at[w, step], mate_recv.at[w], here.mate).wait_send()
        blocks_of(w, core)[0].wait_send()
        blocks_of(w, other)[0].wait_recv()


def store_kernel(*refs):
    held, whole, sem = refs[:3], refs[3:6], refs[6]
    copies = [
        pltpu.make_async_copy(a.at[layer, x], b.at[layer, x], sem.at[i, layer, x])
        for i, (a, b) in enumerate(zip(held, whole))
        for layer in range(2)
        for x in range(2)
    ]
    for copy in copies:
        copy.start()
    for copy in copies:
        copy.wait()


def dma(*shape):
    return pltpu.SemaphoreType.DMA(shape)


def solution(mesh):
    n = len(STREAMS)

    def summed(terms):
        blocks = [t.shape[5:] for t in terms]
        return pl.pallas_call(
            sum_kernel,
            out_shape=[jax.ShapeDtypeStruct((2, *b), BF16) for b in blocks] + [jax.ShapeDtypeStruct((8, 128), F32)],
            in_specs=[pl.BlockSpec(memory_space=pl.ANY)] * 3,
            out_specs=[pl.BlockSpec(memory_space=pl.ANY)] * 3 + [pl.BlockSpec(memory_space=pltpu.VMEM)],
            scratch_shapes=[pltpu.VMEM((16, *part_shape(part, blocks[which])), BF16) for which, part, _ in STREAMS] * 3
            + [pltpu.VMEM(b, BF16) for b in blocks]
            + [pltpu.VMEM((DEVICES, 8, 128), F32)]
            + [dma(n, 16), dma(n), dma(n, 16), dma(n), dma(n, 16)]
            + [dma(n)] * 3
            + [dma()] * 2,
            compiler_params=pltpu.CompilerParams(collective_id=0, has_side_effects=True, vmem_limit_bytes=67_043_328),
            name="sum_terms",
        )(*terms)

    def gathered(rows):
        blocks = [(2 * r.shape[1], r.shape[2]) for r in rows]
        return pl.pallas_call(
            gather_kernel,
            out_shape=[jax.ShapeDtypeStruct((2, 2, 2, 2, 2, *b), BF16) for b in blocks],
            in_specs=[pl.BlockSpec(memory_space=pltpu.VMEM)] * 3,
            out_specs=[pl.BlockSpec(memory_space=pl.ANY)] * 3,
            scratch_shapes=[pltpu.VMEM(r.shape[1:], BF16) for r in rows]
            + [pltpu.VMEM(b, BF16) for b in blocks]
            + [pltpu.VMEM(blocks[2], F32)]
            + [dma(3)] * 2
            + [dma(n, 4), dma(n, 16), dma(n), dma(n)]
            + [dma(3)],
            compiler_params=pltpu.CompilerParams(collective_id=1, has_side_effects=True, vmem_limit_bytes=10 * 2**20),
            name="gather_weights",
        )(*rows)

    def stored(held):
        return pl.pallas_call(
            store_kernel,
            out_shape=[jax.ShapeDtypeStruct(h.shape, h.dtype) for h in held],
            in_specs=[pl.BlockSpec(memory_space=pl.ANY)] * 3,
            out_specs=[pl.BlockSpec(memory_space=pl.ANY)] * 3,
            scratch_shapes=[dma(3, 2, 2)],
            compiler_params=pltpu.CompilerParams(vmem_limit_bytes=2**20),
            name="store_weights",
        )(*held)

    def step(*arrays):
        terms, weights, m, v = (arrays[i : i + 3] for i in (0, 3, 6, 9))
        me = lax.axis_index("dp")
        core = lax.rem(me, 2)
        *sums, squares = summed([t[0].reshape(2, 2, 2, 2, 2, -1, t.shape[3]) for t in terms])
        count = sum(w.size for w in weights)
        factor = jnp.minimum(1.0, 0.5 * lax.rsqrt(squares[0, 0] / count + 1e-30))

        def cut(array, index, size):
            return lax.dynamic_slice_in_dim(array, index * size, size, 1).astype(F32)

        new = [adamw(cut(w, me, m.shape[1]), m, v, cut(g, core, m.shape[1]) * factor) for w, m, v, g in zip(weights, m, v, sums, strict=True)]
        whole = [one.reshape(w.shape) for one, w in zip(stored(gathered([one[0] for one in new])), weights, strict=True)]
        return (*whole, *(one[1] for one in new), *(one[2] for one in new))

    all_of, cut_of = P(None, None, None), P(None, "dp", None)
    return jax.shard_map(
        step,
        mesh=mesh,
        in_specs=(P(("rep", "dp"), None, None, None),) * 3 + (all_of,) * 3 + (cut_of,) * 6,
        out_specs=(P("rep", None, None),) * 3 + (P("rep", "dp", None),) * 6,
        check_vma=False,
    )
```

```python
import functools

import jax
import jax.numpy as jnp
from jax import lax
from jax.experimental import pallas as pl
from jax.experimental.pallas import tpu as pltpu
from jax.sharding import PartitionSpec as P

MESH = pl.DeviceIdType.MESH
F32, BF16 = jnp.float32, jnp.bfloat16

X, Y, Z1, Z0 = range(4)
DEVICES = 32
CHIP_BITS = (16, 8, 4, 2)
STREAMS = ((0, None, (X, Y, Z0, Z1)), (1, None, (Y, X, Z0, Z1)), (2, 0, (Z0, X, Y, Z1)), (2, 1, (Z0, Y, X, Z1)))
ORDERS = [order for _, _, order in STREAMS]
SUM = (
    61, 29, 15, 9, 63, 43, 31, 55, 59, 11, 46, 57, 13, 62, 40, 26, 7, 53, 47, 51, 23, 45, 30, 5, 39, 3, 14, 60, 49, 42, 21, 27, 38, 58,
    56, 41, 44, 54, 52, 22, 37, 1, 10, 35, 50, 25, 8, 6, 19, 33, 28, 12, 2, 36, 18, 34, 24, 17, 20, 4, 48, 32, 0, 16,
)
GATHER = (
    77, 64, 66, 68, 78, 70, 65, 79, 75, 73, 69, 74, 49, 2, 72, 4, 33, 18, 34, 52, 20, 71, 50, 17, 51, 35, 12, 67, 22, 26, 6, 42, 53,
    19, 1, 39, 10, 76, 55, 3, 38, 5, 8, 25, 21, 7, 28, 30, 37, 46, 40, 14, 27, 9, 47, 54, 11, 23, 36, 43, 60, 63, 24, 45, 13, 29, 15,
    44, 56, 61, 58, 59, 62, 57, 41, 31,
)
SUM = tuple(divmod(entry, 16) for entry in SUM)
GATHER = tuple(divmod(entry, 16) if entry < 64 else (entry // 4 - 16, None, entry % 4) for entry in GATHER)
STEP_OF = {s: 4 - s.bit_length() for s in range(1, 16)}


def adamw(w, m, v, g):
    m = 0.9 * m + 0.1 * g
    v = 0.95 * v + 0.05 * g * g
    step = m * lax.rsqrt(v + 1e-8) + 0.1 * w
    return (w - 0.02 * step).astype(BF16), m, v


STORE_REFS = ((0, 3), (3, 2), (5, 3), (8, 2), (10, 2), (12, 2), (14, 1), (15, 1), (16, 1))


class Place:
    def __init__(self):
        me = self.me = lax.axis_index("dp")
        self.core = lax.rem(me, 2)
        self.other = 1 - self.core
        self.bits = [lax.rem(lax.div(me, bit), 2) for bit in CHIP_BITS]
        self.partner = [{"dp": me + bit * (1 - 2 * b)} for bit, b in zip(CHIP_BITS, self.bits)]
        self.mate = {"dp": me + 1 - 2 * self.core}

    def block(self, order, slot):
        at = list(self.bits)
        for step, bit in enumerate(order):
            if slot >> (3 - step) & 1:
                at[bit] = 1 - at[bit]
        return tuple(at)

    def nth(self, k):
        return {"dp": lax.rem(self.me + k, DEVICES)}

    def greet(self):
        barrier = pltpu.get_barrier_semaphore()
        for device in (*self.partner, self.mate):
            pl.semaphore_signal(barrier, inc=1, device_id=device, device_id_type=MESH)
        pl.semaphore_wait(barrier, 5)


def columns(part, shape):
    half = shape[1] // 2
    return slice(None) if part is None else pl.ds(part * half, half)


def part_shape(part, shape):
    return shape if part is None else (shape[0], shape[1] // 2)


def remote(src, dst, send, recv, device):
    return pltpu.make_async_remote_copy(src_ref=src, dst_ref=dst, send_sem=send, recv_sem=recv, device_id=device, device_id_type=MESH)


def pieces(shape):
    rows, columns = shape
    if rows % 16 == 0:
        return rows // 16, lambda i: (pl.ds(pl.multiple_of(i * 16, 16), 16), slice(None))
    return columns // 128, lambda i: (slice(None), pl.ds(pl.multiple_of(i * 128, 128), 128))


def sum_kernel(*refs):
    n = len(STREAMS)
    refs = iter(refs)
    take = lambda count: [next(refs) for _ in range(count)]
    terms, sums, (squares,) = take(3), take(3), take(1)
    own, mate, got, final = take(n), take(n), take(n), take(3)
    parts, own_sem, mate_send, mate_recv, send, recv, out_sem, out_send, out_recv, sq_send, sq_recv = refs
    here = Place()
    core, other = here.core, here.other
    def term(w, layer, s):
        which, part, order = STREAMS[w]
        ref = terms[which]
        return ref.at[(layer, *here.block(order, s), slice(None), columns(part, ref.shape[5:]))]

    def own_copy(w, s):
        return pltpu.make_async_copy(term(w, core, s), own[w].at[s], own_sem.at[w, s])

    def mate_copy(w, s):
        return remote(term(w, other, s), mate[w].at[s], mate_send.at[w], mate_recv.at[w, s], here.mate)

    def result(w):
        which, part, _ = STREAMS[w]
        return final[which].at[:, columns(part, final[which].shape)]

    def home(w, layer):
        which, part, _ = STREAMS[w]
        return sums[which].at[layer, :, columns(part, final[which].shape)]

    def keep(w):
        return pltpu.make_async_copy(result(w), home(w, core), out_sem.at[w])

    def swap(w):
        return remote(result(w), home(w, core), out_send.at[w], out_recv.at[w], here.mate)

    def from_swap(w):
        return remote(home(w, other), home(w, other), out_send.at[w], out_recv.at[w], here.mate)

    def hop(w, s):
        return remote(own[w].at[s], got[w].at[s], send.at[w], recv.at[w, s], here.partner[ORDERS[w][STEP_OF[s]]])

    for w, s in SUM[:16]:
        own_copy(w, s).start()
    here.greet()
    for w, s in SUM:
        mate_copy(w, s).start()
    for w, s in SUM[16:]:
        own_copy(w, s).start()

    squares[...] = jnp.zeros_like(squares)
    last = min(SUM.index((w, 0)) for w in range(n))
    for turn, (w, s) in enumerate(SUM):
        if turn == last:
            for stream in range(n):
                remote(mate[stream], mate[stream], mate_send.at[stream], mate_recv.at[stream, 0], here.mate).wait_send()
        own_copy(w, s).wait()
        mate_copy(w, s).wait_recv()
        arrived = [s + b for b in (8, 4, 2, 1) if s < b]
        for a in arrived:
            hop(w, a).wait_recv()
        count, piece = pieces(own[w].shape[1:])

        def total(i):
            at = (s, *piece(i))
            so_far = own[w][at].astype(F32) + mate[w][at].astype(F32)
            for a in arrived:
                so_far = so_far + got[w][(a, *piece(i))].astype(F32)
            return so_far.astype(BF16)

        if s:

            def body(i, _):
                own[w][(s, *piece(i))] = total(i)
                return _

            lax.fori_loop(0, count, body, 0)
            hop(w, s).start()
        else:

            def body(i, _):
                value = total(i)
                target = result(w)
                target[piece(i)] = value
                value = value.astype(F32)
                value = (value * value).reshape(-1, 8, value.shape[1]).sum(0)
                squares[...] += sum(value[:, j : j + 128] for j in range(0, value.shape[1], 128))
                return _

            lax.fori_loop(0, count, body, 0)
            keep(w).start()
            swap(w).start()

    me = here.me
    parts[me] = squares[...]

    def part_to(k):
        return remote(parts.at[me], parts.at[me], sq_send, sq_recv, here.nth(k))

    def start(k, _):
        part_to(k).start()
        return _

    lax.fori_loop(1, DEVICES, start, 0)
    for w in range(n):
        from_swap(w).wait_recv()
        keep(w).wait()
        swap(w).wait_send()
        sent = own[w].at[pl.ds(1, 15)]
        remote(sent, sent, send.at[w], recv.at[w, 0], here.mate).wait_send()
    others = parts.at[pl.ds(0, DEVICES - 1)]
    remote(others, others, sq_send, sq_recv, here.mate).wait()
    squares[...] = jnp.full_like(squares, jnp.sum(parts[...]))


def gather_kernel(*refs):
    n = len(STREAMS)
    refs = iter(refs)
    take = lambda: [next(refs) for _ in range(3)]
    rows, whole, theirs, block = take(), take(), take(), take()
    wide, row_send, row_recv, send, recv, mate_send, mate_recv, own_sem = refs
    here = Place()
    core, other = here.core, here.other
    here.greet()

    def swap(w):
        return remote(rows[w].at[other], theirs[w], row_send.at[w], row_recv.at[w], here.mate)

    def place(w, s, layer):
        which, part, order = STREAMS[w]
        ref = whole[which]
        return ref.at[(layer, *here.block(order, s), slice(None), columns(part, ref.shape[5:]))]

    def source(w, s):
        which, part, _ = STREAMS[w]
        return place(w, s, core) if s else block[which].at[:, columns(part, block[which].shape)]

    def hop(w, s, step):
        a = s + (8 >> step)
        return remote(source(w, s), place(w, s, core), send.at[w, step], recv.at[w, a], here.partner[ORDERS[w][step]])

    def arrival(w, s):
        target = place(w, s, core)
        return remote(target, target, send.at[w, 0], recv.at[w, s], here.partner[ORDERS[w][STEP_OF[s]]])

    def across(w, s):
        return remote(source(w, s), place(w, s, core), mate_send.at[w], mate_recv.at[w], here.mate)

    def blocks_of(w, layer, *cut):
        which, part, _ = STREAMS[w]
        free = (slice(None),) * (5 - len(cut))
        ref = whole[which].at[(layer, *cut, *free, columns(part, whole[which].shape[5:]))]
        return remote(ref, ref, mate_send.at[w], mate_recv.at[w], here.mate), ref

    def keep(w):
        return pltpu.make_async_copy(block[w], whole[w].at[(core, *here.bits)], own_sem.at[w])

    for w in range(3):
        swap(w).start()
    for w in range(3):
        swap(w).wait_recv()
        half = rows[w].shape[1]
        mine, his = rows[w][core], theirs[w][...]
        low, high = jnp.where(core == 0, mine, his), jnp.where(core == 0, his, mine)
        if half % 16 == 0:
            block[w][:half] = low
            block[w][half:] = high
        else:
            wide[:half] = low.astype(F32)
            wide[half:] = high.astype(F32)
            block[w][...] = wide[...].astype(BF16)
    first = True
    for w, s, *step in GATHER:
        if step:
            hop(w, 0, *step).start()
            continue
        if first:
            for stream in range(n):
                across(stream, 0).start()
            for weight in range(3):
                keep(weight).start()
            first = False
        arrival(w, s).wait_recv()
        for step in reversed(range(STEP_OF[s])):
            hop(w, s, step).start()
        across(w, s).start()
    for w in range(3):
        swap(w).wait_send()
        keep(w).wait()
    for w in range(n):
        for step in range(4):
            _, ref = blocks_of(w, core, *[0] * (step + 1))
            remote(ref, ref, send.at[w, step], mate_recv.at[w], here.mate).wait_send()
        blocks_of(w, core)[0].wait_send()
        blocks_of(w, other)[0].wait_recv()


def store_kernel(*refs):
    held, moments, whole, turned, flat, middle, sem, in_sem, out_sem = (refs[i : i + n] for i, n in STORE_REFS)
    (sem,), (in_sem,), (out_sem,) = sem, in_sem, out_sem
    copies = [
        pltpu.make_async_copy(a.at[layer, x], b.at[layer, x], sem.at[i, layer, x])
        for i, (a, b) in enumerate(zip(held, whole))
        for layer in range(2)
        for x in range(2)
    ]
    inward = [pltpu.make_async_copy(a, b, in_sem.at[i]) for i, (a, b) in enumerate(zip(moments, flat))]
    outward = [pltpu.make_async_copy(a, b, out_sem.at[i]) for i, (a, b) in enumerate(zip(middle, turned))]
    for copy in (*inward, *copies):
        copy.start()
    for i in range(2):
        inward[i].wait()
        for layer in range(2):
            middle[i][:, layer, :] = flat[i][layer]
        outward[i].start()
    for copy in (*copies, *outward):
        copy.wait()


def dma(*shape):
    return pltpu.SemaphoreType.DMA(shape)


def solution(mesh):
    n = len(STREAMS)

    def summed(terms):
        blocks = [t.shape[5:] for t in terms]
        return pl.pallas_call(
            sum_kernel,
            out_shape=[jax.ShapeDtypeStruct((2, *b), BF16) for b in blocks] + [jax.ShapeDtypeStruct((8, 128), F32)],
            in_specs=[pl.BlockSpec(memory_space=pl.ANY)] * 3,
            out_specs=[pl.BlockSpec(memory_space=pl.ANY)] * 3 + [pl.BlockSpec(memory_space=pltpu.VMEM)],
            scratch_shapes=[pltpu.VMEM((16, *part_shape(part, blocks[which])), BF16) for which, part, _ in STREAMS] * 3
            + [pltpu.VMEM(b, BF16) for b in blocks]
            + [pltpu.VMEM((DEVICES, 8, 128), F32)]
            + [dma(n, 16), dma(n), dma(n, 16), dma(n), dma(n, 16)]
            + [dma(n)] * 3
            + [dma()] * 2,
            compiler_params=pltpu.CompilerParams(collective_id=0, has_side_effects=True, vmem_limit_bytes=67_043_328),
            name="sum_terms",
        )(*terms)

    def gathered(rows):
        blocks = [(2 * r.shape[1], r.shape[2]) for r in rows]
        return pl.pallas_call(
            gather_kernel,
            out_shape=[jax.ShapeDtypeStruct((2, 2, 2, 2, 2, *b), BF16) for b in blocks],
            in_specs=[pl.BlockSpec(memory_space=pltpu.VMEM)] * 3,
            out_specs=[pl.BlockSpec(memory_space=pl.ANY)] * 3,
            scratch_shapes=[pltpu.VMEM(r.shape[1:], BF16) for r in rows]
            + [pltpu.VMEM(b, BF16) for b in blocks]
            + [pltpu.VMEM(blocks[2], F32)]
            + [dma(3)] * 2
            + [dma(n, 4), dma(n, 16), dma(n), dma(n)]
            + [dma(3)],
            compiler_params=pltpu.CompilerParams(collective_id=1, has_side_effects=True, vmem_limit_bytes=10 * 2**20),
            name="gather_weights",
        )(*rows)

    def stored(held, moments):
        turned = [jax.ShapeDtypeStruct((m.shape[1], m.shape[0], m.shape[2]), F32) for m in moments]
        return pl.pallas_call(
            store_kernel,
            out_shape=[jax.ShapeDtypeStruct(h.shape, h.dtype) for h in held] + turned,
            in_specs=[pl.BlockSpec(memory_space=pl.ANY)] * 5,
            out_specs=[pl.BlockSpec(memory_space=pl.ANY)] * 5,
            scratch_shapes=[pltpu.VMEM(m.shape, F32) for m in moments] + [pltpu.VMEM(t.shape, F32) for t in turned] + [dma(3, 2, 2), dma(2), dma(2)],
            compiler_params=pltpu.CompilerParams(vmem_limit_bytes=6 * 2**20),
            name="store_weights",
        )(*held, *moments)

    def step(*arrays):
        terms, weights, m, v = (arrays[i : i + 3] for i in (0, 3, 6, 9))
        me = lax.axis_index("dp")
        core = lax.rem(me, 2)
        *sums, squares = summed([t[0].reshape(2, 2, 2, 2, 2, -1, t.shape[3]) for t in terms])
        count = sum(w.size for w in weights)
        factor = jnp.minimum(1.0, 0.5 * lax.rsqrt(squares[0, 0] / count + 1e-30))

        def cut(array, index, size):
            return lax.dynamic_slice_in_dim(array, index * size, size, 1).astype(F32)

        new = [adamw(cut(w, me, m.shape[1]), m, v, cut(g, core, m.shape[1]) * factor) for w, m, v, g in zip(weights, m, v, sums, strict=True)]
        *held, m_down, v_down = stored(gathered([one[0] for one in new]), new[2][1:])
        whole = [one.reshape(w.shape) for one, w in zip(held, weights, strict=True)]
        m_down, v_down = (jnp.transpose(one, (1, 0, 2)) for one in (m_down, v_down))
        return (*whole, new[0][1], new[1][1], m_down, new[0][2], new[1][2], v_down)

    all_of, cut_of = P(None, None, None), P(None, "dp", None)
    return jax.shard_map(
        step,
        mesh=mesh,
        in_specs=(P(("rep", "dp"), None, None, None),) * 3 + (all_of,) * 3 + (cut_of,) * 6,
        out_specs=(P("rep", None, None),) * 3 + (P("rep", "dp", None),) * 6,
        check_vma=False,
    )
```

```python
import functools

import jax
import jax.numpy as jnp
from jax import lax
from jax.experimental import pallas as pl
from jax.experimental.pallas import tpu as pltpu
from jax.sharding import PartitionSpec as P

MESH = pl.DeviceIdType.MESH
F32, BF16 = jnp.float32, jnp.bfloat16

X, Y, Z1, Z0 = range(4)
DEVICES = 32
CHIP_BITS = (16, 8, 4, 2)
STREAMS = ((0, None, (X, Y, Z0, Z1)), (1, None, (Y, X, Z0, Z1)), (2, 0, (Z0, X, Y, Z1)), (2, 1, (Z0, Y, X, Z1)))
ORDERS = [order for _, _, order in STREAMS]
SUM = (
    61, 29, 15, 9, 63, 43, 31, 55, 59, 11, 46, 57, 13, 62, 40, 26, 7, 53, 47, 51, 23, 45, 30, 5, 39, 3, 14, 60, 49, 42, 21, 27, 38, 58,
    56, 41, 44, 54, 52, 22, 37, 1, 10, 35, 50, 25, 8, 6, 19, 33, 28, 12, 2, 36, 18, 34, 24, 17, 20, 4, 48, 32, 0, 16,
)
GATHER = (
    77, 64, 66, 68, 78, 70, 65, 79, 75, 73, 69, 74, 49, 2, 72, 4, 33, 18, 34, 52, 20, 71, 50, 17, 51, 35, 12, 67, 22, 26, 6, 42, 53,
    19, 1, 39, 10, 76, 55, 3, 38, 5, 8, 25, 21, 7, 28, 30, 37, 46, 40, 14, 27, 9, 47, 54, 11, 23, 36, 43, 60, 63, 24, 45, 13, 29, 15,
    44, 56, 61, 58, 59, 62, 57, 41, 31,
)
SUM = tuple(divmod(entry, 16) for entry in SUM)
GATHER = tuple(divmod(entry, 16) if entry < 64 else (entry // 4 - 16, None, entry % 4) for entry in GATHER)
STEP_OF = {s: 4 - s.bit_length() for s in range(1, 16)}


def adamw(w, m, v, g):
    m = 0.9 * m + 0.1 * g
    v = 0.95 * v + 0.05 * g * g
    step = m * lax.rsqrt(v + 1e-8) + 0.1 * w
    return (w - 0.02 * step).astype(BF16), m, v


STORE_REFS = ((0, 3), (3, 2), (5, 3), (8, 2), (10, 2), (12, 2), (14, 1), (15, 1), (16, 1))

EARLY = next(i for i, entry in enumerate(GATHER) if len(entry) == 2)


class Place:
    def __init__(self):
        me = self.me = lax.axis_index("dp")
        self.core = lax.rem(me, 2)
        self.other = 1 - self.core
        self.bits = [lax.rem(lax.div(me, bit), 2) for bit in CHIP_BITS]
        self.partner = [{"dp": me + bit * (1 - 2 * b)} for bit, b in zip(CHIP_BITS, self.bits)]
        self.mate = {"dp": me + 1 - 2 * self.core}

    def block(self, order, slot):
        at = list(self.bits)
        for step, bit in enumerate(order):
            if slot >> (3 - step) & 1:
                at[bit] = 1 - at[bit]
        return tuple(at)

    def nth(self, k):
        return {"dp": lax.rem(self.me + k, DEVICES)}

    def greet(self):
        barrier = pltpu.get_barrier_semaphore()
        for device in (*self.partner, self.mate):
            pl.semaphore_signal(barrier, inc=1, device_id=device, device_id_type=MESH)
        pl.semaphore_wait(barrier, 5)


def columns(part, shape):
    half = shape[1] // 2
    return slice(None) if part is None else pl.ds(part * half, half)


def part_shape(part, shape):
    return shape if part is None else (shape[0], shape[1] // 2)


def remote(src, dst, send, recv, device):
    return pltpu.make_async_remote_copy(src_ref=src, dst_ref=dst, send_sem=send, recv_sem=recv, device_id=device, device_id_type=MESH)


def pieces(shape):
    rows, columns = shape
    if rows % 16 == 0:
        return rows // 16, lambda i: (pl.ds(pl.multiple_of(i * 16, 16), 16), slice(None))
    return columns // 128, lambda i: (slice(None), pl.ds(pl.multiple_of(i * 128, 128), 128))


def sum_kernel(*refs):
    n = len(STREAMS)
    refs = iter(refs)
    take = lambda count: [next(refs) for _ in range(count)]
    terms, sums, (squares,) = take(3), take(3), take(1)
    own, mate, got, final = take(n), take(n), take(n), take(3)
    parts, own_sem, mate_send, mate_recv, send, recv, out_sem, out_send, out_recv, sq_send, sq_recv = refs
    here = Place()
    core, other = here.core, here.other
    def term(w, layer, s):
        which, part, order = STREAMS[w]
        ref = terms[which]
        return ref.at[(layer, *here.block(order, s), slice(None), columns(part, ref.shape[5:]))]

    def own_copy(w, s):
        return pltpu.make_async_copy(term(w, core, s), own[w].at[s], own_sem.at[w, s])

    def mate_copy(w, s):
        return remote(term(w, other, s), mate[w].at[s], mate_send.at[w], mate_recv.at[w, s], here.mate)

    def result(w):
        which, part, _ = STREAMS[w]
        return final[which].at[:, columns(part, final[which].shape)]

    def home(w, layer):
        which, part, _ = STREAMS[w]
        return sums[which].at[layer, :, columns(part, final[which].shape)]

    def keep(w):
        return pltpu.make_async_copy(result(w), home(w, core), out_sem.at[w])

    def swap(w):
        return remote(result(w), home(w, core), out_send.at[w], out_recv.at[w], here.mate)

    def from_swap(w):
        return remote(home(w, other), home(w, other), out_send.at[w], out_recv.at[w], here.mate)

    def hop(w, s):
        return remote(own[w].at[s], got[w].at[s], send.at[w], recv.at[w, s], here.partner[ORDERS[w][STEP_OF[s]]])

    for w, s in SUM[:16]:
        own_copy(w, s).start()
    here.greet()
    for w, s in SUM:
        mate_copy(w, s).start()
    for w, s in SUM[16:]:
        own_copy(w, s).start()

    squares[...] = jnp.zeros_like(squares)
    last = min(SUM.index((w, 0)) for w in range(n))
    for turn, (w, s) in enumerate(SUM):
        if turn == last:
            for stream in range(n):
                remote(mate[stream], mate[stream], mate_send.at[stream], mate_recv.at[stream, 0], here.mate).wait_send()
        own_copy(w, s).wait()
        mate_copy(w, s).wait_recv()
        arrived = [s + b for b in (8, 4, 2, 1) if s < b]
        for a in arrived:
            hop(w, a).wait_recv()
        count, piece = pieces(own[w].shape[1:])

        def total(i):
            at = (s, *piece(i))
            so_far = own[w][at].astype(F32) + mate[w][at].astype(F32)
            for a in arrived:
                so_far = so_far + got[w][(a, *piece(i))].astype(F32)
            return so_far.astype(BF16)

        if s:

            def body(i, _):
                own[w][(s, *piece(i))] = total(i)
                return _

            lax.fori_loop(0, count, body, 0)
            hop(w, s).start()
        else:

            def body(i, _):
                value = total(i)
                target = result(w)
                target[piece(i)] = value
                value = value.astype(F32)
                value = (value * value).reshape(-1, 8, value.shape[1]).sum(0)
                squares[...] += sum(value[:, j : j + 128] for j in range(0, value.shape[1], 128))
                return _

            lax.fori_loop(0, count, body, 0)
            keep(w).start()
            swap(w).start()

    me = here.me
    parts[me] = squares[...]

    def part_to(k):
        return remote(parts.at[me], parts.at[me], sq_send, sq_recv, here.nth(k))

    def start(k, _):
        part_to(k).start()
        return _

    lax.fori_loop(1, DEVICES, start, 0)
    for w in range(n):
        from_swap(w).wait_recv()
        keep(w).wait()
        swap(w).wait_send()
        sent = own[w].at[pl.ds(1, 15)]
        remote(sent, sent, send.at[w], recv.at[w, 0], here.mate).wait_send()
    others = parts.at[pl.ds(0, DEVICES - 1)]
    remote(others, others, sq_send, sq_recv, here.mate).wait()
    squares[...] = jnp.full_like(squares, jnp.sum(parts[...]))


def gather_kernel(*refs):
    n = len(STREAMS)
    refs = iter(refs)
    take = lambda: [next(refs) for _ in range(3)]
    rows, whole, theirs, block = take(), take(), take(), take()
    wide, row_send, row_recv, send, recv, mate_send, mate_recv, own_sem = refs
    here = Place()
    core, other = here.core, here.other
    here.greet()

    def swap(w):
        return remote(rows[w].at[other], theirs[w], row_send.at[w], row_recv.at[w], here.mate)

    def place(w, s, layer):
        which, part, order = STREAMS[w]
        ref = whole[which]
        return ref.at[(layer, *here.block(order, s), slice(None), columns(part, ref.shape[5:]))]

    def source(w, s):
        which, part, _ = STREAMS[w]
        return place(w, s, core) if s else block[which].at[:, columns(part, block[which].shape)]

    def hop(w, s, step):
        a = s + (8 >> step)
        return remote(source(w, s), place(w, s, core), send.at[w, step], recv.at[w, a], here.partner[ORDERS[w][step]])

    def arrival(w, s):
        target = place(w, s, core)
        return remote(target, target, send.at[w, 0], recv.at[w, s], here.partner[ORDERS[w][STEP_OF[s]]])

    def across(w, s):
        return remote(source(w, s), place(w, s, core), mate_send.at[w], mate_recv.at[w], here.mate)

    def blocks_of(w, layer, *cut):
        which, part, _ = STREAMS[w]
        free = (slice(None),) * (5 - len(cut))
        ref = whole[which].at[(layer, *cut, *free, columns(part, whole[which].shape[5:]))]
        return remote(ref, ref, mate_send.at[w], mate_recv.at[w], here.mate), ref

    def keep(w):
        return pltpu.make_async_copy(block[w], whole[w].at[(core, *here.bits)], own_sem.at[w])

    for w in range(3):
        swap(w).start()
    for w in range(3):
        swap(w).wait_recv()
        half = rows[w].shape[1]
        mine, his = rows[w][core], theirs[w][...]
        low, high = jnp.where(core == 0, mine, his), jnp.where(core == 0, his, mine)
        if half % 16 == 0:
            block[w][:half] = low
            block[w][half:] = high
        else:
            wide[:half] = low.astype(F32)
            wide[half:] = high.astype(F32)
            block[w][...] = wide[...].astype(BF16)
        for stream, _, *step in GATHER[:EARLY]:
            if STREAMS[stream][0] == w:
                hop(stream, 0, *step).start()
    first = True
    for w, s, *step in GATHER[EARLY:]:
        if step:
            hop(w, 0, *step).start()
            continue
        if first:
            for stream in range(n):
                across(stream, 0).start()
            for weight in range(3):
                keep(weight).start()
            first = False
        arrival(w, s).wait_recv()
        for step in reversed(range(STEP_OF[s])):
            hop(w, s, step).start()
        across(w, s).start()
    for w in range(3):
        swap(w).wait_send()
        keep(w).wait()
    for w in range(n):
        for step in range(4):
            _, ref = blocks_of(w, core, *[0] * (step + 1))
            remote(ref, ref, send.at[w, step], mate_recv.at[w], here.mate).wait_send()
        blocks_of(w, core)[0].wait_send()
        blocks_of(w, other)[0].wait_recv()


def store_kernel(*refs):
    held, moments, whole, turned, flat, middle, sem, in_sem, out_sem = (refs[i : i + n] for i, n in STORE_REFS)
    (sem,), (in_sem,), (out_sem,) = sem, in_sem, out_sem
    copies = [
        pltpu.make_async_copy(a.at[layer, x], b.at[layer, x], sem.at[i, layer, x])
        for i, (a, b) in enumerate(zip(held, whole))
        for layer in range(2)
        for x in range(2)
    ]
    inward = [pltpu.make_async_copy(a, b, in_sem.at[i]) for i, (a, b) in enumerate(zip(moments, flat))]
    outward = [pltpu.make_async_copy(a, b, out_sem.at[i]) for i, (a, b) in enumerate(zip(middle, turned))]
    for copy in (*inward, *copies):
        copy.start()
    for i in range(2):
        inward[i].wait()
        for layer in range(2):
            middle[i][:, layer, :] = flat[i][layer]
        outward[i].start()
    for copy in (*copies, *outward):
        copy.wait()


def dma(*shape):
    return pltpu.SemaphoreType.DMA(shape)


def solution(mesh):
    n = len(STREAMS)

    def summed(terms):
        blocks = [t.shape[5:] for t in terms]
        return pl.pallas_call(
            sum_kernel,
            out_shape=[jax.ShapeDtypeStruct((2, *b), BF16) for b in blocks] + [jax.ShapeDtypeStruct((8, 128), F32)],
            in_specs=[pl.BlockSpec(memory_space=pl.ANY)] * 3,
            out_specs=[pl.BlockSpec(memory_space=pl.ANY)] * 3 + [pl.BlockSpec(memory_space=pltpu.VMEM)],
            scratch_shapes=[pltpu.VMEM((16, *part_shape(part, blocks[which])), BF16) for which, part, _ in STREAMS] * 3
            + [pltpu.VMEM(b, BF16) for b in blocks]
            + [pltpu.VMEM((DEVICES, 8, 128), F32)]
            + [dma(n, 16), dma(n), dma(n, 16), dma(n), dma(n, 16)]
            + [dma(n)] * 3
            + [dma()] * 2,
            compiler_params=pltpu.CompilerParams(collective_id=0, has_side_effects=True, vmem_limit_bytes=67_043_328),
            name="sum_terms",
        )(*terms)

    def gathered(rows):
        blocks = [(2 * r.shape[1], r.shape[2]) for r in rows]
        return pl.pallas_call(
            gather_kernel,
            out_shape=[jax.ShapeDtypeStruct((2, 2, 2, 2, 2, *b), BF16) for b in blocks],
            in_specs=[pl.BlockSpec(memory_space=pltpu.VMEM)] * 3,
            out_specs=[pl.BlockSpec(memory_space=pl.ANY)] * 3,
            scratch_shapes=[pltpu.VMEM(r.shape[1:], BF16) for r in rows]
            + [pltpu.VMEM(b, BF16) for b in blocks]
            + [pltpu.VMEM(blocks[2], F32)]
            + [dma(3)] * 2
            + [dma(n, 4), dma(n, 16), dma(n), dma(n)]
            + [dma(3)],
            compiler_params=pltpu.CompilerParams(collective_id=1, has_side_effects=True, vmem_limit_bytes=10 * 2**20),
            name="gather_weights",
        )(*rows)

    def stored(held, moments):
        turned = [jax.ShapeDtypeStruct((m.shape[1], m.shape[0], m.shape[2]), F32) for m in moments]
        return pl.pallas_call(
            store_kernel,
            out_shape=[jax.ShapeDtypeStruct(h.shape, h.dtype) for h in held] + turned,
            in_specs=[pl.BlockSpec(memory_space=pl.ANY)] * 5,
            out_specs=[pl.BlockSpec(memory_space=pl.ANY)] * 5,
            scratch_shapes=[pltpu.VMEM(m.shape, F32) for m in moments] + [pltpu.VMEM(t.shape, F32) for t in turned] + [dma(3, 2, 2), dma(2), dma(2)],
            compiler_params=pltpu.CompilerParams(vmem_limit_bytes=6 * 2**20),
            name="store_weights",
        )(*held, *moments)

    def step(*arrays):
        terms, weights, m, v = (arrays[i : i + 3] for i in (0, 3, 6, 9))
        me = lax.axis_index("dp")
        core = lax.rem(me, 2)
        *sums, squares = summed([t[0].reshape(2, 2, 2, 2, 2, -1, t.shape[3]) for t in terms])
        count = sum(w.size for w in weights)
        factor = jnp.minimum(1.0, 0.5 * lax.rsqrt(squares[0, 0] / count + 1e-30))

        def cut(array, index, size):
            return lax.dynamic_slice_in_dim(array, index * size, size, 1).astype(F32)

        new = [adamw(cut(w, me, m.shape[1]), m, v, cut(g, core, m.shape[1]) * factor) for w, m, v, g in zip(weights, m, v, sums, strict=True)]
        *held, m_down, v_down = stored(gathered([one[0] for one in new]), new[2][1:])
        whole = [one.reshape(w.shape) for one, w in zip(held, weights, strict=True)]
        m_down, v_down = (jnp.transpose(one, (1, 0, 2)) for one in (m_down, v_down))
        return (*whole, new[0][1], new[1][1], m_down, new[0][2], new[1][2], v_down)

    all_of, cut_of = P(None, None, None), P(None, "dp", None)
    return jax.shard_map(
        step,
        mesh=mesh,
        in_specs=(P(("rep", "dp"), None, None, None),) * 3 + (all_of,) * 3 + (cut_of,) * 6,
        out_specs=(P("rep", None, None),) * 3 + (P("rep", "dp", None),) * 6,
        check_vma=False,
    )
```
